32 devices in a mesh: grp: 8 (over z, x), node: 4 (over y, core).
Axes of the slice: x: 2, y: 2, z: 4, core: 2. Of those that a mesh axis runs over, the one named last changes fastest.
Arguments:
- initial: float32 [6, 32, 32768], P(None, None, ('grp', 'node')), may hold values from -0.5 to 16, as said below
- afferent_noise_level: float32 [32, 32768], P(None, ('grp', 'node')), may hold values from 0.12 to 0.32
- history: bfloat16 [64, 32, 32768], P(None, None, ('grp', 'node')), may hold values from 0 to 1
- weights: bfloat16 [32, 24, 128, 1024], P(('grp', 'node')), may hold values from -0.109375 to 0.109375
- lead_field: bfloat16 [128, 32768], P(None, ('grp', 'node')), may hold values from -0.00390625 to 0.00390625
- src_group: int32 [32, 24], replicated, may hold values from 0 to 7, as said below
- src_sub: int32 [32, 24], replicated, may hold values from 0 to 7
- delays: int32 [32, 24], replicated, may hold values from 6 to 63
- counts: int32 [32], replicated, may hold values from 16 to 24, as said below
Outputs:
- final_state: float32 [6, 32, 32768], P(None, None, ('grp', 'node'))
- sensors: float32 [6, 128, 32], replicated
The draws below stay inside these ranges and needn't reach their ends.
Inputs may be any that keep to these rules, and one draw needn't show every extreme that they name: `initial`: rows 0 to 2 are potentials and rows 3 to 5 their rates; row 0 lies within 0 and 0.4, row 1 within 4 and 16, row 2 within 0 and 8, rows 3 to 5 within -0.5 and 0.5. `src_group`: among the tiles k < counts[b] of a block b no owner group appears more than 3 times, and some block reaches 3. Tiles k >= counts[b] of block b are ignored; in every draw some block has 24 live tiles.
All inputs are finite; a program needn't handle non-finite values.
Results may differ from the reference program's by a relative error of at most 0.0003.
The reference program's roundings to bfloat16 on the way (of `cycle` and `potential`) count: a program that leaves them out, or rounds other values in their place, can miss the bound.
Values may be sent and summed in bfloat16 or wider, within the bound.
A program may use at most 128 MiB of HBM per device.

```python
import math
import jax
import jax.numpy as jnp
from jax import lax

BLOCK = 1024
SUB = 128
KMAX = 24
CYCLE = 64
DMIN = 6
STEPS = 6
SENS = 128
REPS = 32
OWNERS = 8
COLUMNS = 4
BLOCKS = 32
NODES = 32768
CAP = 3
PIECES = 8


def draw_initial(key, part):
    keys = jax.random.split(key, 6)
    shape = (REPS, NODES)
    lows = (0.0, 4.0, 0.0, -0.5, -0.5, -0.5)
    highs = (0.4, 16.0, 8.0, 0.5, 0.5, 0.5)
    rows = []
    for row_index in range(6):
        unit = jax.random.uniform(keys[row_index], shape, jnp.float32)
        rows.append(lows[row_index] + (highs[row_index] - lows[row_index]) * unit)
    return jnp.stack(rows)


def draw_src_group(key, part):
    keys = jax.random.split(key, BLOCKS)

    def one_row(row_key):
        order = jax.random.permutation(row_key, CAP * OWNERS)
        return (order[:KMAX] % OWNERS).astype(jnp.int32)
    return jax.vmap(one_row)(keys)


def draw_counts(key, part):
    first_key, second_key = jax.random.split(key)
    base_counts = jax.random.randint(first_key, (BLOCKS,), KMAX - KMAX // 3, KMAX + 1)
    full_block = jax.random.randint(second_key, (), 0, BLOCKS)
    return base_counts.at[full_block].set(KMAX).astype(jnp.int32)


def place_ends(array, own_key, smallest, top_value):
    longest = array.shape.index(max(array.shape))
    spots = []
    for shift in (0, 1):
        where = [jax.random.randint(jax.random.fold_in(own_key, axis), (), 0, length) for axis, length in enumerate(array.shape)]
        where[longest] = (where[longest] + shift) % array.shape[longest]
        spots.append(tuple(where))
    return array.at[spots[0]].set(smallest).at[spots[1]].set(top_value)


def levels(own_key, extent, cuts, smallest, largest):
    def one(position, blocks):
        heights = jax.random.uniform(jax.random.fold_in(jax.random.fold_in(own_key, 6), position), (blocks,), jnp.float32, smallest / len(cuts), largest / len(cuts))
        return jnp.repeat(jnp.exp(heights), extent[position] // blocks).reshape((-1,) + (1,) * (len(extent) - position - 1))

    loudness = one(*cuts[0])
    for cut in cuts[1:]:
        loudness = loudness * one(*cut)
    return loudness


def gaussian(own_key, dims, width, limit, cuts=(), kind=jnp.bfloat16):
    drawn = width * jax.random.normal(own_key, dims, jnp.float32)
    if cuts:
        drawn = drawn * levels(own_key, dims, cuts, -0.22, 0.18)
    return jnp.clip(drawn, -limit, limit).astype(kind)


def setup_inputs(seed: int = 0) -> dict:
    splits = jax.random.split(jax.random.key(seed), 10)
    initial = draw_initial(jax.random.fold_in(splits[9], 71), 0)
    afferent_noise_level = jnp.clip(jnp.exp(math.log(0.32) - 0.98082925 * jax.random.uniform(splits[1], (REPS, NODES), jnp.float32) ** levels(splits[1], (REPS, NODES), ((1, 32),), -0.2, 0.2)), 0.12, 0.32)
    history = jnp.clip(1.0 * jax.random.uniform(splits[2], (CYCLE, REPS, NODES), jnp.float32) ** levels(splits[2], (CYCLE, REPS, NODES), ((2, 32),), -0.2, 0.2), 0.0, 1.0).astype(jnp.bfloat16)
    weights = gaussian(splits[3], (BLOCKS, KMAX, SUB, BLOCK), (KMAX * SUB) ** -0.5, 0.109375, ((0, 32),))
    lead_field = gaussian(splits[4], (SENS, NODES), (64 * NODES) ** -0.5, 0.00390625, ((1, 32),))
    src_group = draw_src_group(jax.random.fold_in(splits[9], 71), 0)
    src_sub = place_ends(jax.random.randint(splits[6], (BLOCKS, KMAX), 0, PIECES), jax.random.fold_in(splits[6], 1), 0, PIECES - 1).astype(jnp.int32)
    delays = place_ends(jax.random.randint(splits[7], (BLOCKS, KMAX), DMIN, CYCLE), jax.random.fold_in(splits[7], 1), DMIN, CYCLE - 1).astype(jnp.int32)
    counts = draw_counts(jax.random.fold_in(splits[9], 71), 0)
    return dict(initial=initial, afferent_noise_level=afferent_noise_level, history=history, weights=weights, lead_field=lead_field, src_group=src_group, src_sub=src_sub, delays=delays, counts=counts)


exciting_amplitude = 3.25
suppressive_amplitude = 22.0
exciting_inverse_lag = 0.1
suppressive_inverse_lag = 0.05
link_factor = 135.0
maximal_spike_frequency = 0.005
thresh = 6.0
fire_slope = 0.56
global_scaling_factor = 0.5
dt_step = 0.5


def sigmoid_spike_density(somatic_charge_level):
    return 1.0 / (1.0 + jnp.exp(fire_slope * (thresh - somatic_charge_level)))


def derivative(population_variables, afferent_noise_level, network_afferent):
    principal_cell_level, interneuron_depolarization, suppressive_depolarization = population_variables[0], population_variables[1], population_variables[2]
    principal_cell_curvature = exciting_amplitude * exciting_inverse_lag * maximal_spike_frequency * sigmoid_spike_density(interneuron_depolarization - suppressive_depolarization) - 2.0 * exciting_inverse_lag * population_variables[3] - exciting_inverse_lag * exciting_inverse_lag * principal_cell_level
    interneuron_second_derivative = exciting_amplitude * exciting_inverse_lag * (afferent_noise_level + 0.8 * link_factor * maximal_spike_frequency * sigmoid_spike_density(link_factor * principal_cell_level) + global_scaling_factor * network_afferent) - 2.0 * exciting_inverse_lag * population_variables[4] - exciting_inverse_lag * exciting_inverse_lag * interneuron_depolarization
    suppressive_second_derivative = suppressive_amplitude * suppressive_inverse_lag * 0.25 * link_factor * maximal_spike_frequency * sigmoid_spike_density(0.25 * link_factor * principal_cell_level) - 2.0 * suppressive_inverse_lag * population_variables[5] - suppressive_inverse_lag * suppressive_inverse_lag * suppressive_depolarization
    return jnp.stack([population_variables[3], population_variables[4], population_variables[5], principal_cell_curvature, interneuron_second_derivative, suppressive_second_derivative])


def advance(population_variables, afferent_noise_level, coupled_now, coupled_next):
    first_rate = derivative(population_variables, afferent_noise_level, coupled_now)
    second_rate = derivative(population_variables + dt_step * first_rate, afferent_noise_level, coupled_next)
    return population_variables + (0.5 * dt_step) * (first_rate + second_rate)


def gather_input(cycle, in_time, weights, src_group, src_sub, delays, counts):
    zero_index = jnp.zeros((), jnp.int32)
    tile_lanes = jnp.arange(KMAX, dtype=jnp.int32)
    column = jnp.arange(BLOCKS, dtype=jnp.int32) % COLUMNS
    starts = ((src_group * COLUMNS + column[:, None]) * BLOCK + src_sub * SUB).astype(jnp.int32)
    slot_ids = jnp.mod(in_time - delays, CYCLE).astype(jnp.int32)

    def cut_piece(slot_id, start_id):
        return lax.dynamic_slice(cycle, (slot_id, zero_index, start_id), (1, REPS, SUB))[0]

    def one_block(element):
        start_row, slot_row, live_count, tile_block = element
        pieces = jax.vmap(cut_piece)(slot_row, start_row)
        live_mask = (tile_lanes < live_count).astype(jnp.bfloat16)
        pieces = pieces * live_mask[:, None, None]
        flattened = jnp.transpose(pieces, (1, 0, 2)).reshape(REPS, KMAX * SUB)
        return jnp.dot(flattened, tile_block.reshape(KMAX * SUB, BLOCK), preferred_element_type=jnp.float32)

    products = lax.map(one_block, (starts, slot_ids, counts, weights), batch_size=8)
    return jnp.transpose(products, (1, 0, 2)).reshape(REPS, BLOCKS * BLOCK)


def reference(initial, afferent_noise_level, history, weights, lead_field, src_group, src_sub, delays, counts):
    zero_index = jnp.zeros((), jnp.int32)

    def inputs(cycle, in_time):
        return gather_input(cycle, in_time, weights, src_group, src_sub, delays, counts)

    def record(sensors, population_variables, step_id):
        potential = (population_variables[1] - population_variables[2]).astype(jnp.bfloat16)
        local_sum = lax.dot_general(lead_field, potential, (((1,), (1,)), ((), ())), preferred_element_type=jnp.float32)
        return lax.dynamic_update_slice(sensors, local_sum[None], (step_id, zero_index, zero_index))

    network_afferent = inputs(history, jnp.zeros((), jnp.int32))
    sensors = jnp.zeros((STEPS, SENS, REPS), jnp.float32)

    def one_step(step_id, carried):
        population_variables, cycle, coupled_now, sensors = carried
        step_id = jnp.asarray(step_id).astype(jnp.int32)
        spike_density_result = sigmoid_spike_density(population_variables[1] - population_variables[2]).astype(jnp.bfloat16)
        cycle = lax.dynamic_update_slice(cycle, spike_density_result[None], (jnp.mod(step_id, CYCLE).astype(jnp.int32), zero_index, zero_index))
        coupled_next = inputs(cycle, step_id + 1)
        population_variables = advance(population_variables, afferent_noise_level, coupled_now, coupled_next)
        return population_variables, cycle, coupled_next, record(sensors, population_variables, step_id)

    population_variables, cycle, network_afferent, sensors = lax.fori_loop(0, STEPS, one_step, (initial, history, network_afferent, sensors))
    return population_variables, sensors
```

```python
import functools

import jax
import jax.numpy as jnp
from jax import lax
from jax.experimental import pallas as pl
from jax.experimental.pallas import tpu as pltpu
from jax.sharding import PartitionSpec as P

DMIN = 6
STEPS = 6
TIMES = STEPS + 1
BULK = 4
INNER = 2
WINDOW = TIMES
VMEM_BYTES = 40 * 1024 * 1024

exciting_amplitude = 3.25
suppressive_amplitude = 22.0
exciting_inverse_lag = 0.1
suppressive_inverse_lag = 0.05
link_factor = 135.0
maximal_spike_frequency = 0.005
thresh = 6.0
fire_slope = 0.56
global_scaling_factor = 0.5
dt_step = 0.5

COUPLED_RATE = exciting_amplitude * exciting_inverse_lag * global_scaling_factor
NEXT_GAIN = 0.5 * dt_step * COUPLED_RATE
POTENTIAL_GAIN = (
    0.5
    * dt_step
    * (2.0 * NEXT_GAIN + dt_step * (COUPLED_RATE - 2.0 * exciting_inverse_lag * NEXT_GAIN))
)

MESH = pl.DeviceIdType.MESH


def sigmoid_spike_density(level):
    return 1.0 / (1.0 + jnp.exp(fire_slope * (thresh - level)))


def derivative(y, noise, coupled):
    curvature = (
        exciting_amplitude
        * exciting_inverse_lag
        * maximal_spike_frequency
        * sigmoid_spike_density(y[1] - y[2])
        - 2.0 * exciting_inverse_lag * y[3]
        - exciting_inverse_lag * exciting_inverse_lag * y[0]
    )
    drive = noise + 0.8 * link_factor * maximal_spike_frequency * sigmoid_spike_density(
        link_factor * y[0]
    )
    if coupled is not None:
        drive = drive + global_scaling_factor * coupled
    interneuron = (
        exciting_amplitude * exciting_inverse_lag * drive
        - 2.0 * exciting_inverse_lag * y[4]
        - exciting_inverse_lag * exciting_inverse_lag * y[1]
    )
    suppressive = (
        suppressive_amplitude
        * suppressive_inverse_lag
        * 0.25
        * link_factor
        * maximal_spike_frequency
        * sigmoid_spike_density(0.25 * link_factor * y[0])
        - 2.0 * suppressive_inverse_lag * y[5]
        - suppressive_inverse_lag * suppressive_inverse_lag * y[2]
    )
    return [y[3], y[4], y[5], curvature, interneuron, suppressive]


def advance(y, noise, coupled_now):
    first = derivative(y, noise, coupled_now)
    moved = [a + dt_step * b for a, b in zip(y, first)]
    second = derivative(moved, noise, None)
    return [a + 0.5 * dt_step * (b + c) for a, b, c in zip(y, first, second)]


def flip(index, mask):
    out = index
    bit = 1
    while bit <= mask:
        if mask & bit:
            out = out + bit * (1 - 2 * (lax.div(index, bit) % 2))
        bit *= 2
    return out


def kernel(
    owners,
    columns,
    slots,
    src_group,
    src_sub,
    delays,
    counts,
    initial_hbm,
    noise_hbm,
    history_hbm,
    weights_hbm,
    lead_hbm,
    final_out,
    sensors_out,
    sel_sub,
    sel_start,
    sel_tile,
    hist,
    state,
    noise,
    weights,
    placed,
    lead,
    lead_t,
    staged,
    landed,
    coupled,
    base,
    potential,
    bulk,
    bulk_in,
    bulk_z,
    bulk_all,
    full_in,
    full_z,
    local_sem,
    past_sem,
    send_sem,
    recv_sem,
    bulk_send,
    bulk_recv,
    bulk_z_send,
    bulk_z_recv,
    bulk_all_send,
    bulk_all_recv,
    full_send,
    full_recv,
    full_z_send,
    full_z_recv,
):
    me = lax.axis_index("grp")
    column = lax.axis_index("node")
    outer = owners // INNER
    layer = lax.div(me, INNER)
    inside = lax.rem(me, INNER)
    near = INNER * columns
    seat = inside * columns + column
    tiles = src_group.shape[0]
    cycle_len, replicas, block_len = history_hbm.shape
    piece_len = weights.shape[1]
    share = bulk.shape[1]

    loads = [
        pltpu.make_async_copy(initial_hbm, state, local_sem.at[0]),
        pltpu.make_async_copy(weights_hbm, weights.at[pl.ds(0, tiles)], local_sem.at[1]),
        pltpu.make_async_copy(noise_hbm, noise, local_sem.at[2]),
        pltpu.make_async_copy(lead_hbm, lead, local_sem.at[3]),
    ]
    past = [
        pltpu.make_async_copy(
            history_hbm.at[:, :, pl.ds(i * piece_len, piece_len)],
            hist.at[pl.ds(0, cycle_len), i],
            past_sem.at[i],
        )
        for i in range(block_len // piece_len)
    ]
    loads[0].start()
    for copy in past:
        copy.start()

    def partner(p, d):
        return flip(layer, p) * INNER + lax.rem(inside + d, INNER)

    pairs = [(p, d) for p in range(outer - 1, -1, -1) for d in range(INNER)]
    remote = [(p, d) for p, d in pairs if (p, d) != (0, 0)]
    seats = [(d, c) for d in range(INNER) for c in range(columns) if (d, c) != (0, 0)]

    barrier = pltpu.get_barrier_semaphore()
    for p, d in remote:
        pl.semaphore_signal(
            barrier, inc=1, device_id={"grp": partner(p, d)}, device_id_type=MESH
        )
    for d, c in seats:
        if c:
            pl.semaphore_signal(
                barrier,
                inc=1,
                device_id={"grp": partner(0, d), "node": lax.rem(column + c, columns)},
                device_id_type=MESH,
            )
    greeted = len(remote) + len([1 for d, c in seats if c])
    for copy in loads[1:]:
        copy.start()

    def choose(block, owner):
        live = counts[block]
        rank = jnp.int32(0)
        found = [jnp.int32(tiles)] * slots
        subs = [jnp.int32(0)] * slots
        starts = [jnp.int32(cycle_len - DMIN)] * slots
        for k in range(tiles):
            hit = jnp.logical_and(src_group[k, block] == owner, k < live)
            sub, start = src_sub[k, block], cycle_len - delays[k, block]
            for r in range(slots):
                take = jnp.logical_and(hit, rank == r)
                found[r] = jnp.where(take, k, found[r])
                subs[r] = jnp.where(take, sub, subs[r])
                starts[r] = jnp.where(take, start, starts[r])
            rank = rank + jnp.where(hit, 1, 0)
        return found, subs, starts

    def choose_out(dest, carry):
        _, subs, starts = choose(dest * columns + column, me)
        for r in range(slots):
            sel_sub[dest * slots + r] = subs[r]
            sel_start[dest * slots + r] = starts[r]
        return carry

    lax.fori_loop(0, owners, choose_out, 0)

    loads[0].wait()

    def first_fire(tile, carry):
        cols = pl.ds(pl.multiple_of(tile * piece_len, piece_len), piece_len)
        fire = sigmoid_spike_density(state[1, :, cols] - state[2, :, cols])
        hist[cycle_len, tile] = fire.astype(jnp.bfloat16)
        return carry

    lax.fori_loop(0, block_len // piece_len, first_fire, 0)
    for copy in past:
        copy.wait()

    def pack(place, carry):
        start, sub = sel_start[place], sel_sub[place]
        for t in range(TIMES):
            staged[t, place] = hist[start + t, sub]
        return carry

    lax.fori_loop(0, owners * slots, pack, 0)

    mine = pl.ds(me * slots, slots)

    def parcel(t, p, d):
        dest = partner(p, d)
        return pltpu.make_async_remote_copy(
            src_ref=staged.at[t, pl.ds(dest * slots, slots)],
            dst_ref=landed.at[t, mine],
            send_sem=send_sem.at[t, p * INNER + d],
            recv_sem=recv_sem.at[t, p * INNER + d],
            device_id={"grp": dest},
            device_id_type=MESH,
        )

    pl.semaphore_wait(barrier, greeted)
    for t in range(WINDOW):
        for p, d in remote:
            parcel(t, p, d).start()

    def keep(t, carry):
        landed[t, mine] = staged[t, mine]
        return carry

    lax.fori_loop(0, TIMES, keep, 0)

    def choose_in(owner, carry):
        found, _, _ = choose(me * columns + column, owner)
        for r in range(slots):
            sel_tile[owner * slots + r] = found[r]
        return carry

    lax.fori_loop(0, owners, choose_in, 0)
    weights[tiles] = jnp.zeros(weights.shape[1:], jnp.bfloat16)
    loads[1].wait()

    def place_weights(place, carry):
        rows = pl.ds(pl.multiple_of(place * piece_len, piece_len), piece_len)
        placed[rows, :] = weights[sel_tile[place]]
        return carry

    lax.fori_loop(0, owners * slots, place_weights, 0)
    loads[2].wait()
    loads[3].wait()
    lead_t[...] = lead[...].T

    group = INNER * slots
    depth = group * piece_len
    dot_cols = min(512, block_len)

    def absorb(t, p):
        for d in range(INNER):
            if (p, d) != (0, 0):
                parcel(t, p, d).wait_recv()
        zone = flip(layer, p)
        lhs = jnp.concatenate([landed[t, zone * group + i] for i in range(group)], axis=1)
        rows = pl.ds(pl.multiple_of(zone * depth, depth), depth)
        for start in range(0, block_len, dot_cols):
            cols = slice(start, start + dot_cols)
            part = jnp.dot(lhs, placed[rows, cols], preferred_element_type=jnp.float32)
            if p == 0:
                coupled[:, cols] = part
            else:
                coupled[:, cols] = coupled[:, cols] + part

    part_rows = 16

    def blocks(body):
        def step(i, carry):
            rows = pl.ds(pl.multiple_of(lax.rem(i, replicas // part_rows) * part_rows, part_rows), part_rows)
            cols = pl.ds(
                pl.multiple_of(lax.div(i, replicas // part_rows) * piece_len, piece_len), piece_len
            )
            body(rows, cols)
            return carry

        lax.fori_loop(0, (replicas // part_rows) * (block_len // piece_len), step, 0)

    def read(rows, cols):
        return [state[i, rows, cols] for i in range(6)]

    def move(t, out):
        def body(rows, cols):
            y = read(rows, cols)
            now = coupled[rows, cols]
            if t > 0:
                y[4] = y[4] + NEXT_GAIN * now
            y = advance(y, noise[rows, cols], now)
            if out is state:
                potential[rows, cols] = (y[1] - y[2]).astype(jnp.bfloat16)
            for i in range(6):
                out[i, rows, cols] = y[i]

        blocks(body)

    def signal():
        return jnp.dot(potential[...], lead_t[...], preferred_element_type=jnp.float32)

    def near_device(d, c):
        return {"grp": partner(0, d), "node": lax.rem(column + c, columns)}

    def full_copy(s, d, c):
        return pltpu.make_async_remote_copy(
            src_ref=full_in.at[s, seat],
            dst_ref=full_in.at[s, seat],
            send_sem=full_send.at[s, d * columns + c],
            recv_sem=full_recv.at[s, d * columns + c],
            device_id=near_device(d, c),
            device_id_type=MESH,
        )

    def full_z_copy(s, p):
        return pltpu.make_async_remote_copy(
            src_ref=full_z.at[s, layer],
            dst_ref=full_z.at[s, layer],
            send_sem=full_z_send.at[s, p],
            recv_sem=full_z_recv.at[s, p],
            device_id={"grp": partner(p, 0)},
            device_id_type=MESH,
        )

    def bulk_copy(d, c):
        other = lax.rem(inside + d, INNER) * columns + lax.rem(column + c, columns)
        return pltpu.make_async_remote_copy(
            src_ref=bulk.at[other],
            dst_ref=bulk_in.at[seat],
            send_sem=bulk_send.at[d * columns + c],
            recv_sem=bulk_recv.at[d * columns + c],
            device_id=near_device(d, c),
            device_id_type=MESH,
        )

    def bulk_z_copy(p):
        return pltpu.make_async_remote_copy(
            src_ref=bulk_z.at[layer],
            dst_ref=bulk_z.at[layer],
            send_sem=bulk_z_send.at[p],
            recv_sem=bulk_z_recv.at[p],
            device_id={"grp": partner(p, 0)},
            device_id_type=MESH,
        )

    def bulk_all_copy(d, c):
        return pltpu.make_async_remote_copy(
            src_ref=bulk_all.at[seat],
            dst_ref=bulk_all.at[seat],
            send_sem=bulk_all_send.at[d * columns + c],
            recv_sem=bulk_all_recv.at[d * columns + c],
            device_id=near_device(d, c),
            device_id_type=MESH,
        )

    def total(ref, count):
        out = ref[0]
        for i in range(1, count):
            out = out + ref[i]
        return out

    layers = list(range(1, outer))

    def start_full(s):
        full_in[s, seat] = signal()
        for d, c in seats:
            full_copy(s, d, c).start()

    def turn_full(s):
        for d, c in seats:
            full_copy(s, d, c).wait_recv()
        full_z[s, layer] = total(full_in.at[s], near)
        for p in layers:
            full_z_copy(s, p).start()

    def end_full(s):
        for p in layers:
            full_z_copy(s, p).wait_recv()
        row = (BULK + s) * replicas
        sensors_out[row : row + replicas, :] = total(full_z.at[s], outer)

    for t in range(BULK):
        for p in range(outer):
            absorb(t, p)
        move(t, state)
        part = signal()
        for i in range(replicas // share):
            bulk[t * (replicas // share) + i] = part[i * share : (i + 1) * share, :]
    for d, c in seats:
        bulk_copy(d, c).start()
    bulk_in[seat] = bulk[seat]

    t = BULK
    for p in range(outer):
        absorb(t, p)
    move(t, state)
    start_full(0)
    for d, c in seats:
        bulk_copy(d, c).wait_recv()
    bulk_z[layer] = total(bulk_in, near)
    for p in layers:
        bulk_z_copy(p).start()

    def ahead(rows, cols):
        y = read(rows, cols)
        y = advance(y, noise[rows, cols], None)
        base[rows, cols] = y[1] - y[2]

    blocks(ahead)

    t = BULK + 1
    for p in range(outer):
        absorb(t, p)
    potential[...] = (base[...] + POTENTIAL_GAIN * coupled[...]).astype(jnp.bfloat16)
    start_full(1)

    turn_full(0)
    for p in layers:
        bulk_z_copy(p).wait_recv()
    bulk_all[seat] = total(bulk_z, outer)
    for d, c in seats:
        bulk_all_copy(d, c).start()
    move(t, final_out)

    t = BULK + 2
    absorb(t, 0)
    turn_full(1)
    for p in range(1, outer):
        absorb(t, p)
    final_out[4] = final_out[4] + NEXT_GAIN * coupled[...]

    end_full(0)
    for d, c in seats:
        bulk_all_copy(d, c).wait_recv()
    for i in range(near):
        sensors_out[i * share : (i + 1) * share, :] = bulk_all[i]
    for t in range(TIMES):
        for p, d in remote:
            parcel(t, p, d).wait_send()
    for d, c in seats:
        bulk_copy(d, c).wait_send()
        bulk_all_copy(d, c).wait_send()
        for s in range(2):
            full_copy(s, d, c).wait_send()
    for p in layers:
        bulk_z_copy(p).wait_send()
        full_z_copy(0, p).wait_send()
    end_full(1)
    for p in layers:
        full_z_copy(1, p).wait_send()


def deliver(state, sensors, state_out, sensors_out, sem):
    copies = [
        pltpu.make_async_copy(sensors, sensors_out, sem.at[0]),
        pltpu.make_async_copy(state, state_out, sem.at[1]),
    ]
    for copy in copies:
        copy.start()
    for copy in copies:
        copy.wait()


def body(
    owners,
    columns,
    initial,
    afferent_noise_level,
    history,
    weights,
    lead_field,
    src_group,
    src_sub,
    delays,
    counts,
):
    cycle_len, replicas, block_len = history.shape
    tiles = src_group.shape[1]
    piece_len = weights.shape[2]
    sensors = lead_field.shape[0]
    slots = (tiles + owners - 1) // owners
    places = owners * slots
    outer = owners // INNER
    near = INNER * columns
    share = BULK * replicas // near
    smem = pl.BlockSpec(memory_space=pltpu.SMEM)
    vmem = pl.BlockSpec(memory_space=pltpu.VMEM)
    anywhere = pl.BlockSpec(memory_space=pl.ANY)
    dma = pltpu.SemaphoreType.DMA
    final, signal = pl.pallas_call(
        functools.partial(kernel, owners, columns, slots),
        out_shape=(
            pltpu.VMEM(initial.shape, jnp.float32),
            pltpu.VMEM((STEPS * replicas, sensors), jnp.float32),
        ),
        in_specs=[smem] * 4 + [pl.BlockSpec(memory_space=pltpu.HBM)] * 5,
        out_specs=(vmem, vmem),
        scratch_shapes=[
            pltpu.SMEM((places,), jnp.int32),
            pltpu.SMEM((places,), jnp.int32),
            pltpu.SMEM((places,), jnp.int32),
            pltpu.VMEM((cycle_len + 1, block_len // piece_len, replicas, piece_len), jnp.bfloat16),
            pltpu.VMEM(initial.shape, jnp.float32),
            pltpu.VMEM((replicas, block_len), jnp.float32),
            pltpu.VMEM((tiles + 1, piece_len, block_len), jnp.bfloat16),
            pltpu.VMEM((places * piece_len, block_len), jnp.bfloat16),
            pltpu.VMEM(lead_field.shape, jnp.bfloat16),
            pltpu.VMEM((block_len, sensors), jnp.bfloat16),
            pltpu.VMEM((TIMES, places, replicas, piece_len), jnp.bfloat16),
            pltpu.VMEM((TIMES, places, replicas, piece_len), jnp.bfloat16),
            pltpu.VMEM((replicas, block_len), jnp.float32),
            pltpu.VMEM((replicas, block_len), jnp.float32),
            pltpu.VMEM((replicas, block_len), jnp.bfloat16),
            pltpu.VMEM((near, share, sensors), jnp.float32),
            pltpu.VMEM((near, share, sensors), jnp.float32),
            pltpu.VMEM((outer, share, sensors), jnp.float32),
            pltpu.VMEM((near, share, sensors), jnp.float32),
            pltpu.VMEM((2, near, replicas, sensors), jnp.float32),
            pltpu.VMEM((2, outer, replicas, sensors), jnp.float32),
            dma((4,)),
            dma((block_len // piece_len,)),
            dma((TIMES, owners)),
            dma((TIMES, owners)),
            dma((near,)),
            dma((near,)),
            dma((outer,)),
            dma((outer,)),
            dma((near,)),
            dma((near,)),
            dma((2, near)),
            dma((2, near)),
            dma((2, outer)),
            dma((2, outer)),
        ],
        compiler_params=pltpu.CompilerParams(
            collective_id=0, has_side_effects=True, vmem_limit_bytes=VMEM_BYTES
        ),
    )(
        *(
            pltpu.with_memory_space_constraint(array, pltpu.HBM)
            for array in (
                src_group.T,
                src_sub.T,
                delays.T,
                counts,
                initial,
                afferent_noise_level,
                history,
                weights.reshape(tiles, piece_len, block_len),
                lead_field,
            )
        ),
    )
    final, signal = pl.pallas_call(
        deliver,
        out_shape=(
            jax.ShapeDtypeStruct(final.shape, jnp.float32),
            jax.ShapeDtypeStruct(signal.shape, jnp.float32),
        ),
        in_specs=[vmem, vmem],
        out_specs=(anywhere, anywhere),
        scratch_shapes=[dma((2,))],
        compiler_params=pltpu.CompilerParams(vmem_limit_bytes=8 * 1024 * 1024),
    )(
        pltpu.with_memory_space_constraint(final, pltpu.VMEM),
        pltpu.with_memory_space_constraint(signal, pltpu.VMEM),
    )
    signal = signal.reshape(STEPS, replicas, sensors)
    return final, jnp.transpose(signal, (0, 2, 1))


def solution(mesh):
    return jax.shard_map(
        functools.partial(body, mesh.shape["grp"], mesh.shape["node"]),
        mesh=mesh,
        in_specs=(
            P(None, None, ("grp", "node")),
            P(None, ("grp", "node")),
            P(None, None, ("grp", "node")),
            P(("grp", "node"), None, None, None),
            P(None, ("grp", "node")),
            P(),
            P(),
            P(),
            P(),
        ),
        out_specs=(P(None, None, ("grp", "node")), P()),
        check_vma=False,
    )
```

```python
import functools

import jax
import jax.numpy as jnp
from jax import lax
from jax.experimental import pallas as pl
from jax.experimental.pallas import tpu as pltpu
from jax.sharding import PartitionSpec as P

DMIN = 6
STEPS = 6
TIMES = STEPS + 1
BULK = 4
INNER = 2
GROUPS = ((0,), (1, 2), (3,), (4,), (5,), (6,))
AHEAD = 2
STAGE = 2
HOLD = 2
VMEM_BYTES = 40 * 1024 * 1024

exciting_amplitude = 3.25
suppressive_amplitude = 22.0
exciting_inverse_lag = 0.1
suppressive_inverse_lag = 0.05
link_factor = 135.0
maximal_spike_frequency = 0.005
thresh = 6.0
fire_slope = 0.56
global_scaling_factor = 0.5
dt_step = 0.5

COUPLED_RATE = exciting_amplitude * exciting_inverse_lag * global_scaling_factor
NEXT_GAIN = 0.5 * dt_step * COUPLED_RATE
POTENTIAL_GAIN = (
    0.5
    * dt_step
    * (2.0 * NEXT_GAIN + dt_step * (COUPLED_RATE - 2.0 * exciting_inverse_lag * NEXT_GAIN))
)

MESH = pl.DeviceIdType.MESH


def sigmoid_spike_density(level):
    return 1.0 / (1.0 + jnp.exp(fire_slope * (thresh - level)))


def derivative(y, noise, coupled):
    curvature = (
        exciting_amplitude
        * exciting_inverse_lag
        * maximal_spike_frequency
        * sigmoid_spike_density(y[1] - y[2])
        - 2.0 * exciting_inverse_lag * y[3]
        - exciting_inverse_lag * exciting_inverse_lag * y[0]
    )
    drive = noise + 0.8 * link_factor * maximal_spike_frequency * sigmoid_spike_density(
        link_factor * y[0]
    )
    if coupled is not None:
        drive = drive + global_scaling_factor * coupled
    interneuron = (
        exciting_amplitude * exciting_inverse_lag * drive
        - 2.0 * exciting_inverse_lag * y[4]
        - exciting_inverse_lag * exciting_inverse_lag * y[1]
    )
    suppressive = (
        suppressive_amplitude
        * suppressive_inverse_lag
        * 0.25
        * link_factor
        * maximal_spike_frequency
        * sigmoid_spike_density(0.25 * link_factor * y[0])
        - 2.0 * suppressive_inverse_lag * y[5]
        - suppressive_inverse_lag * suppressive_inverse_lag * y[2]
    )
    return [y[3], y[4], y[5], curvature, interneuron, suppressive]


def advance(y, noise, coupled_now):
    first = derivative(y, noise, coupled_now)
    moved = [a + dt_step * b for a, b in zip(y, first)]
    second = derivative(moved, noise, None)
    return [a + 0.5 * dt_step * (b + c) for a, b, c in zip(y, first, second)]


def flip(index, mask):
    out = index
    bit = 1
    while bit <= mask:
        if mask & bit:
            out = out + bit * (1 - 2 * (lax.div(index, bit) % 2))
        bit *= 2
    return out


def kernel(
    owners,
    columns,
    slots,
    group_hbm,
    sub_hbm,
    delays_hbm,
    counts_hbm,
    initial_hbm,
    noise_hbm,
    history_hbm,
    weights_hbm,
    lead_hbm,
    final_out,
    sensors_out,
    src_group,
    src_sub,
    delays,
    counts,
    index_sem,
    sel_sub,
    sel_start,
    sel_tile,
    hist,
    state,
    noise,
    weights,
    placed,
    lead,
    lead_t,
    staged,
    landed,
    coupled,
    base,
    potential,
    bulk,
    bulk_in,
    bulk_z,
    bulk_all,
    full_in,
    full_z,
    local_sem,
    past_sem,
    send_sem,
    recv_sem,
    bulk_send,
    bulk_recv,
    bulk_z_send,
    bulk_z_recv,
    bulk_all_send,
    bulk_all_recv,
    full_send,
    full_recv,
    full_z_send,
    full_z_recv,
):
    me = lax.axis_index("grp")
    column = lax.axis_index("node")
    outer = owners // INNER
    layer = lax.div(me, INNER)
    inside = lax.rem(me, INNER)
    near = INNER * columns
    seat = inside * columns + column
    tiles = src_group.shape[0]
    cycle_len, replicas, block_len = history_hbm.shape
    piece_len = weights.shape[1]
    share = bulk.shape[1]

    def partner(p, d):
        return flip(layer, p) * INNER + lax.rem(inside + d, INNER)

    pairs = [(p, d) for p in range(outer - 1, -1, -1) for d in range(INNER)]
    remote = [(p, d) for p, d in pairs if (p, d) != (0, 0)]
    seats = [(d, c) for d in range(INNER) for c in range(columns) if (d, c) != (0, 0)]

    barrier = pltpu.get_barrier_semaphore()
    for p, d in remote:
        pl.semaphore_signal(
            barrier, inc=1, device_id={"grp": partner(p, d)}, device_id_type=MESH
        )
    for d, c in seats:
        if c:
            pl.semaphore_signal(
                barrier,
                inc=1,
                device_id={"grp": partner(0, d), "node": lax.rem(column + c, columns)},
                device_id_type=MESH,
            )
    loads = [
        pltpu.make_async_copy(initial_hbm, state, local_sem.at[0]),
        pltpu.make_async_copy(weights_hbm, weights.at[pl.ds(0, tiles)], local_sem.at[1]),
        pltpu.make_async_copy(noise_hbm, noise, local_sem.at[2]),
        pltpu.make_async_copy(lead_hbm, lead, local_sem.at[3]),
    ]
    past = [
        pltpu.make_async_copy(
            history_hbm.at[:, :, pl.ds(i * piece_len, piece_len)],
            hist.at[pl.ds(0, cycle_len), i],
            past_sem.at[i],
        )
        for i in range(block_len // piece_len)
    ]
    index = [
        pltpu.make_async_copy(a, b, index_sem.at[i])
        for i, (a, b) in enumerate(
            ((group_hbm, src_group), (sub_hbm, src_sub), (delays_hbm, delays), (counts_hbm, counts))
        )
    ]
    for copy in index:
        copy.start()
    loads[0].start()
    for copy in past:
        copy.start()

    greeted = len(remote) + len([1 for d, c in seats if c])
    for copy in loads[1:]:
        copy.start()

    def choose(block, owner):
        live = counts[block]
        rank = jnp.int32(0)
        found = [jnp.int32(tiles)] * slots
        subs = [jnp.int32(0)] * slots
        starts = [jnp.int32(cycle_len - DMIN)] * slots
        for k in range(tiles):
            hit = jnp.logical_and(src_group[k, block] == owner, k < live)
            sub, start = src_sub[k, block], cycle_len - delays[k, block]
            for r in range(slots):
                take = jnp.logical_and(hit, rank == r)
                found[r] = jnp.where(take, k, found[r])
                subs[r] = jnp.where(take, sub, subs[r])
                starts[r] = jnp.where(take, start, starts[r])
            rank = rank + jnp.where(hit, 1, 0)
        return found, subs, starts

    def choose_out(dest, carry):
        _, subs, starts = choose(dest * columns + column, me)
        for r in range(slots):
            sel_sub[dest * slots + r] = subs[r]
            sel_start[dest * slots + r] = starts[r]
        return carry

    for copy in index:
        copy.wait()
    lax.fori_loop(0, owners, choose_out, 0)

    loads[0].wait()

    def first_fire(tile, carry):
        cols = pl.ds(pl.multiple_of(tile * piece_len, piece_len), piece_len)
        fire = sigmoid_spike_density(state[1, :, cols] - state[2, :, cols])
        hist[cycle_len, tile] = fire.astype(jnp.bfloat16)
        return carry

    lax.fori_loop(0, block_len // piece_len, first_fire, 0)
    for copy in past:
        copy.wait()

    def pack(owner, carry):
        for r in range(slots):
            start, sub = sel_start[owner * slots + r], sel_sub[owner * slots + r]
            for t in range(TIMES):
                staged[owner, t, r] = hist[start + t, sub]
        return carry

    lax.fori_loop(0, owners, pack, 0)

    def parcel(g, p, d):
        times = pl.ds(GROUPS[g][0], len(GROUPS[g]))
        dest = partner(p, d)
        return pltpu.make_async_remote_copy(
            src_ref=staged.at[dest, times],
            dst_ref=landed.at[me, times],
            send_sem=send_sem.at[g, p * INNER + d],
            recv_sem=recv_sem.at[g, p * INNER + d],
            device_id={"grp": dest},
            device_id_type=MESH,
        )

    def issue(g):
        for p, d in remote:
            parcel(g, p, d).start()

    pl.semaphore_wait(barrier, greeted)
    for g in range(AHEAD):
        issue(g)
    landed[me] = staged[me]

    def choose_in(owner, carry):
        found, _, _ = choose(me * columns + column, owner)
        for r in range(slots):
            sel_tile[owner * slots + r] = found[r]
        return carry

    lax.fori_loop(0, owners, choose_in, 0)
    weights[tiles] = jnp.zeros(weights.shape[1:], jnp.bfloat16)
    loads[1].wait()

    def place_weights(place, carry):
        rows = pl.ds(pl.multiple_of(place * piece_len, piece_len), piece_len)
        placed[rows, :] = weights[sel_tile[place]]
        return carry

    lax.fori_loop(0, owners * slots, place_weights, 0)
    loads[2].wait()
    loads[3].wait()
    lead_t[...] = lead[...].T

    group = INNER * slots
    depth = group * piece_len
    dot_cols = min(512, block_len)

    def absorb(g, p):
        for d in range(INNER):
            if (p, d) != (0, 0):
                parcel(g, p, d).wait_recv()
        zone = flip(layer, p)
        lhs = jnp.concatenate(
            [
                jnp.concatenate(
                    [landed[zone * INNER + d, t, r] for d in range(INNER) for r in range(slots)],
                    axis=1,
                )
                for t in GROUPS[g]
            ],
            axis=0,
        )
        out = slice(GROUPS[g][0] * replicas, (GROUPS[g][-1] + 1) * replicas)
        rows = pl.ds(pl.multiple_of(zone * depth, depth), depth)
        for start in range(0, block_len, dot_cols):
            cols = slice(start, start + dot_cols)
            part = jnp.dot(lhs, placed[rows, cols], preferred_element_type=jnp.float32)
            if p == 0:
                coupled[out, cols] = part
            else:
                coupled[out, cols] = coupled[out, cols] + part

    part_rows = 16

    def blocks(body):
        def step(i, carry):
            rows = pl.ds(pl.multiple_of(lax.rem(i, replicas // part_rows) * part_rows, part_rows), part_rows)
            cols = pl.ds(
                pl.multiple_of(lax.div(i, replicas // part_rows) * piece_len, piece_len), piece_len
            )
            body(rows, cols)
            return carry

        lax.fori_loop(0, (replicas // part_rows) * (block_len // piece_len), step, 0)

    def read(rows, cols):
        return [state[i, rows, cols] for i in range(6)]

    def move(t, out):
        def body(rows, cols):
            y = read(rows, cols)
            now = coupled[pl.ds(pl.multiple_of(t * replicas + rows.start, part_rows), part_rows), cols]
            if t > 0:
                y[4] = y[4] + NEXT_GAIN * now
            y = advance(y, noise[rows, cols], now)
            if out is state:
                potential[rows, cols] = (y[1] - y[2]).astype(jnp.bfloat16)
            for i in range(6):
                out[i, rows, cols] = y[i]

        blocks(body)

    def signal():
        return jnp.dot(potential[...], lead_t[...], preferred_element_type=jnp.float32)

    def near_device(d, c):
        return {"grp": partner(0, d), "node": lax.rem(column + c, columns)}

    def full_copy(s, d, c):
        return pltpu.make_async_remote_copy(
            src_ref=full_in.at[s, seat],
            dst_ref=full_in.at[s, seat],
            send_sem=full_send.at[s, d * columns + c],
            recv_sem=full_recv.at[s, d * columns + c],
            device_id=near_device(d, c),
            device_id_type=MESH,
        )

    def full_z_copy(s, p):
        return pltpu.make_async_remote_copy(
            src_ref=full_z.at[s, layer],
            dst_ref=full_z.at[s, layer],
            send_sem=full_z_send.at[s, p],
            recv_sem=full_z_recv.at[s, p],
            device_id={"grp": partner(p, 0)},
            device_id_type=MESH,
        )

    def bulk_copy(d, c):
        other = lax.rem(inside + d, INNER) * columns + lax.rem(column + c, columns)
        return pltpu.make_async_remote_copy(
            src_ref=bulk.at[other],
            dst_ref=bulk_in.at[seat],
            send_sem=bulk_send.at[d * columns + c],
            recv_sem=bulk_recv.at[d * columns + c],
            device_id=near_device(d, c),
            device_id_type=MESH,
        )

    def bulk_z_copy(p):
        return pltpu.make_async_remote_copy(
            src_ref=bulk_z.at[layer],
            dst_ref=bulk_z.at[layer],
            send_sem=bulk_z_send.at[p],
            recv_sem=bulk_z_recv.at[p],
            device_id={"grp": partner(p, 0)},
            device_id_type=MESH,
        )

    def bulk_all_copy(d, c):
        return pltpu.make_async_remote_copy(
            src_ref=bulk_all.at[seat],
            dst_ref=bulk_all.at[seat],
            send_sem=bulk_all_send.at[d * columns + c],
            recv_sem=bulk_all_recv.at[d * columns + c],
            device_id=near_device(d, c),
            device_id_type=MESH,
        )

    def total(ref, count):
        out = ref[0]
        for i in range(1, count):
            out = out + ref[i]
        return out

    layers = list(range(1, outer))

    def start_full(s):
        full_in[s, seat] = signal()
        for d, c in seats:
            full_copy(s, d, c).start()

    def turn_full(s):
        for d, c in seats:
            full_copy(s, d, c).wait_recv()
        full_z[s, layer] = total(full_in.at[s], near)
        for p in layers:
            full_z_copy(s, p).start()

    def end_full(s):
        for p in layers:
            full_z_copy(s, p).wait_recv()
        row = (BULK + s) * replicas
        sensors_out[row : row + replicas, :] = total(full_z.at[s], outer)

    last = len(GROUPS) - 2
    for g in range(last):
        for p in range(outer):
            absorb(g, p)
            if p == STAGE and g + AHEAD <= last:
                issue(g + AHEAD)
        for t in GROUPS[g]:
            move(t, state)
            if t < BULK:
                part = signal()
                for i in range(replicas // share):
                    bulk[t * (replicas // share) + i] = part[i * share : (i + 1) * share, :]
            if t == BULK - 1:
                for d, c in seats:
                    bulk_copy(d, c).start()
                bulk_in[seat] = bulk[seat]
            if t == BULK:
                start_full(0)
                for d, c in seats:
                    bulk_copy(d, c).wait_recv()
                bulk_z[layer] = total(bulk_in, near)
                for p in layers:
                    bulk_z_copy(p).start()

    def ahead(rows, cols):
        y = read(rows, cols)
        y = advance(y, noise[rows, cols], None)
        base[rows, cols] = y[1] - y[2]

    blocks(ahead)
    if HOLD < 0:
        issue(last + 1)

    for p in range(outer):
        absorb(last, p)
        if p == HOLD:
            issue(last + 1)
    at = slice(GROUPS[last][0] * replicas, (GROUPS[last][0] + 1) * replicas)
    potential[...] = (base[...] + POTENTIAL_GAIN * coupled[at, :]).astype(jnp.bfloat16)
    start_full(1)
    if HOLD == outer:
        issue(last + 1)

    turn_full(0)
    for p in layers:
        bulk_z_copy(p).wait_recv()
    bulk_all[seat] = total(bulk_z, outer)
    for d, c in seats:
        bulk_all_copy(d, c).start()
    move(STEPS - 1, final_out)

    absorb(last + 1, 0)
    turn_full(1)
    for p in range(1, outer):
        absorb(last + 1, p)
    at = slice(STEPS * replicas, TIMES * replicas)
    final_out[4] = final_out[4] + NEXT_GAIN * coupled[at, :]

    end_full(0)
    for d, c in seats:
        bulk_all_copy(d, c).wait_recv()
    for i in range(near):
        sensors_out[i * share : (i + 1) * share, :] = bulk_all[i]
    for g in range(len(GROUPS)):
        for p, d in remote:
            parcel(g, p, d).wait_send()
    for d, c in seats:
        bulk_copy(d, c).wait_send()
        bulk_all_copy(d, c).wait_send()
        for s in range(2):
            full_copy(s, d, c).wait_send()
    for p in layers:
        bulk_z_copy(p).wait_send()
        full_z_copy(0, p).wait_send()
    end_full(1)
    for p in layers:
        full_z_copy(1, p).wait_send()


def deliver(state, sensors, state_out, sensors_out, sem):
    copies = [
        pltpu.make_async_copy(sensors, sensors_out, sem.at[0]),
        pltpu.make_async_copy(state, state_out, sem.at[1]),
    ]
    for copy in copies:
        copy.start()
    for copy in copies:
        copy.wait()


def body(
    owners,
    columns,
    initial,
    afferent_noise_level,
    history,
    weights,
    lead_field,
    src_group,
    src_sub,
    delays,
    counts,
):
    cycle_len, replicas, block_len = history.shape
    tiles = src_group.shape[1]
    piece_len = weights.shape[2]
    sensors = lead_field.shape[0]
    slots = (tiles + owners - 1) // owners
    places = owners * slots
    outer = owners // INNER
    near = INNER * columns
    share = BULK * replicas // near
    smem = pl.BlockSpec(memory_space=pltpu.SMEM)
    vmem = pl.BlockSpec(memory_space=pltpu.VMEM)
    anywhere = pl.BlockSpec(memory_space=pl.ANY)
    dma = pltpu.SemaphoreType.DMA
    final, signal = pl.pallas_call(
        functools.partial(kernel, owners, columns, slots),
        out_shape=(
            pltpu.VMEM(initial.shape, jnp.float32),
            pltpu.VMEM((STEPS * replicas, sensors), jnp.float32),
        ),
        in_specs=[pl.BlockSpec(memory_space=pltpu.HBM)] * 9,
        out_specs=(vmem, vmem),
        scratch_shapes=[
            pltpu.SMEM((tiles, src_group.shape[0]), jnp.int32),
            pltpu.SMEM((tiles, src_group.shape[0]), jnp.int32),
            pltpu.SMEM((tiles, src_group.shape[0]), jnp.int32),
            pltpu.SMEM(counts.shape, jnp.int32),
            dma((4,)),
            pltpu.SMEM((places,), jnp.int32),
            pltpu.SMEM((places,), jnp.int32),
            pltpu.SMEM((places,), jnp.int32),
            pltpu.VMEM((cycle_len + 1, block_len // piece_len, replicas, piece_len), jnp.bfloat16),
            pltpu.VMEM(initial.shape, jnp.float32),
            pltpu.VMEM((replicas, block_len), jnp.float32),
            pltpu.VMEM((tiles + 1, piece_len, block_len), jnp.bfloat16),
            pltpu.VMEM((places * piece_len, block_len), jnp.bfloat16),
            pltpu.VMEM(lead_field.shape, jnp.bfloat16),
            pltpu.VMEM((block_len, sensors), jnp.bfloat16),
            pltpu.VMEM((owners, TIMES, slots, replicas, piece_len), jnp.bfloat16),
            pltpu.VMEM((owners, TIMES, slots, replicas, piece_len), jnp.bfloat16),
            pltpu.VMEM((TIMES * replicas, block_len), jnp.float32),
            pltpu.VMEM((replicas, block_len), jnp.float32),
            pltpu.VMEM((replicas, block_len), jnp.bfloat16),
            pltpu.VMEM((near, share, sensors), jnp.float32),
            pltpu.VMEM((near, share, sensors), jnp.float32),
            pltpu.VMEM((outer, share, sensors), jnp.float32),
            pltpu.VMEM((near, share, sensors), jnp.float32),
            pltpu.VMEM((2, near, replicas, sensors), jnp.float32),
            pltpu.VMEM((2, outer, replicas, sensors), jnp.float32),
            dma((4,)),
            dma((block_len // piece_len,)),
            dma((len(GROUPS), owners)),
            dma((len(GROUPS), owners)),
            dma((near,)),
            dma((near,)),
            dma((outer,)),
            dma((outer,)),
            dma((near,)),
            dma((near,)),
            dma((2, near)),
            dma((2, near)),
            dma((2, outer)),
            dma((2, outer)),
        ],
        compiler_params=pltpu.CompilerParams(
            collective_id=0, has_side_effects=True, vmem_limit_bytes=VMEM_BYTES
        ),
    )(
        *(
            pltpu.with_memory_space_constraint(array, pltpu.HBM)
            for array in (
                src_group.T,
                src_sub.T,
                delays.T,
                counts,
                initial,
                afferent_noise_level,
                history,
                weights.reshape(tiles, piece_len, block_len),
                lead_field,
            )
        ),
    )
    final, signal = pl.pallas_call(
        deliver,
        out_shape=(
            jax.ShapeDtypeStruct(final.shape, jnp.float32),
            jax.ShapeDtypeStruct(signal.shape, jnp.float32),
        ),
        in_specs=[vmem, vmem],
        out_specs=(anywhere, anywhere),
        scratch_shapes=[dma((2,))],
        compiler_params=pltpu.CompilerParams(vmem_limit_bytes=8 * 1024 * 1024),
    )(
        pltpu.with_memory_space_constraint(final, pltpu.VMEM),
        pltpu.with_memory_space_constraint(signal, pltpu.VMEM),
    )
    signal = signal.reshape(STEPS, replicas, sensors)
    return final, jnp.transpose(signal, (0, 2, 1))


def solution(mesh):
    return jax.shard_map(
        functools.partial(body, mesh.shape["grp"], mesh.shape["node"]),
        mesh=mesh,
        in_specs=(
            P(None, None, ("grp", "node")),
            P(None, ("grp", "node")),
            P(None, None, ("grp", "node")),
            P(("grp", "node"), None, None, None),
            P(None, ("grp", "node")),
            P(),
            P(),
            P(),
            P(),
        ),
        out_specs=(P(None, None, ("grp", "node")), P()),
        check_vma=False,
    )
```

```python
import functools

import jax
import jax.numpy as jnp
from jax import lax
from jax.experimental import pallas as pl
from jax.experimental.pallas import tpu as pltpu
from jax.sharding import PartitionSpec as P

DMIN = 6
STEPS = 6
TIMES = STEPS + 1
BULK = 4
INNER = 2
GROUPS = ((0,), (1, 2), (3,), (4,), (5,), (6,))
AHEAD = 2
STAGE = 2
HOLD = 2
VMEM_BYTES = 40 * 1024 * 1024

exciting_amplitude = 3.25
suppressive_amplitude = 22.0
exciting_inverse_lag = 0.1
suppressive_inverse_lag = 0.05
link_factor = 135.0
maximal_spike_frequency = 0.005
thresh = 6.0
fire_slope = 0.56
global_scaling_factor = 0.5
dt_step = 0.5

COUPLED_RATE = exciting_amplitude * exciting_inverse_lag * global_scaling_factor
NEXT_GAIN = 0.5 * dt_step * COUPLED_RATE
POTENTIAL_GAIN = (
    0.5
    * dt_step
    * (2.0 * NEXT_GAIN + dt_step * (COUPLED_RATE - 2.0 * exciting_inverse_lag * NEXT_GAIN))
)

MESH = pl.DeviceIdType.MESH


def sigmoid_spike_density(level):
    return 1.0 / (1.0 + jnp.exp(fire_slope * (thresh - level)))


def derivative(y, noise, coupled):
    curvature = (
        exciting_amplitude
        * exciting_inverse_lag
        * maximal_spike_frequency
        * sigmoid_spike_density(y[1] - y[2])
        - 2.0 * exciting_inverse_lag * y[3]
        - exciting_inverse_lag * exciting_inverse_lag * y[0]
    )
    drive = noise + 0.8 * link_factor * maximal_spike_frequency * sigmoid_spike_density(
        link_factor * y[0]
    )
    if coupled is not None:
        drive = drive + global_scaling_factor * coupled
    interneuron = (
        exciting_amplitude * exciting_inverse_lag * drive
        - 2.0 * exciting_inverse_lag * y[4]
        - exciting_inverse_lag * exciting_inverse_lag * y[1]
    )
    suppressive = (
        suppressive_amplitude
        * suppressive_inverse_lag
        * 0.25
        * link_factor
        * maximal_spike_frequency
        * sigmoid_spike_density(0.25 * link_factor * y[0])
        - 2.0 * suppressive_inverse_lag * y[5]
        - suppressive_inverse_lag * suppressive_inverse_lag * y[2]
    )
    return [y[3], y[4], y[5], curvature, interneuron, suppressive]


def advance(y, noise, coupled_now):
    first = derivative(y, noise, coupled_now)
    moved = [a + dt_step * b for a, b in zip(y, first)]
    second = derivative(moved, noise, None)
    return [a + 0.5 * dt_step * (b + c) for a, b, c in zip(y, first, second)]


def flip(index, mask):
    out = index
    bit = 1
    while bit <= mask:
        if mask & bit:
            out = out + bit * (1 - 2 * (lax.div(index, bit) % 2))
        bit *= 2
    return out


def kernel(
    owners,
    columns,
    slots,
    group_hbm,
    sub_hbm,
    delays_hbm,
    counts_hbm,
    initial_hbm,
    noise_hbm,
    history_hbm,
    weights_hbm,
    lead_hbm,
    final_out,
    sensors_out,
    src_group,
    src_sub,
    delays,
    counts,
    index_sem,
    sel_sub,
    sel_start,
    sel_tile,
    hist,
    state,
    noise,
    weights,
    placed,
    lead,
    lead_t,
    staged,
    landed,
    coupled,
    base,
    potential,
    bulk,
    bulk_in,
    bulk_z,
    bulk_all,
    full_in,
    full_z,
    local_sem,
    past_sem,
    send_sem,
    recv_sem,
    bulk_send,
    bulk_recv,
    bulk_z_send,
    bulk_z_recv,
    bulk_all_send,
    bulk_all_recv,
    full_send,
    full_recv,
    full_z_send,
    full_z_recv,
):
    me = lax.axis_index("grp")
    column = lax.axis_index("node")
    outer = owners // INNER
    layer = lax.div(me, INNER)
    inside = lax.rem(me, INNER)
    near = INNER * columns
    seat = inside * columns + column
    tiles = src_group.shape[0]
    cycle_len, replicas, block_len = history_hbm.shape
    piece_len = weights.shape[1]
    share = bulk.shape[1]

    def partner(p, d):
        return flip(layer, p) * INNER + lax.rem(inside + d, INNER)

    pairs = [(p, d) for p in range(outer - 1, -1, -1) for d in range(INNER)]
    remote = [(p, d) for p, d in pairs if (p, d) != (0, 0)]
    seats = [(d, c) for d in range(INNER) for c in range(columns) if (d, c) != (0, 0)]

    barrier = pltpu.get_barrier_semaphore()
    for p, d in remote:
        pl.semaphore_signal(
            barrier, inc=1, device_id={"grp": partner(p, d)}, device_id_type=MESH
        )
    for d, c in seats:
        if c:
            pl.semaphore_signal(
                barrier,
                inc=1,
                device_id={"grp": partner(0, d), "node": lax.rem(column + c, columns)},
                device_id_type=MESH,
            )
    loads = [
        pltpu.make_async_copy(initial_hbm, state, local_sem.at[0]),
        pltpu.make_async_copy(weights_hbm, weights.at[pl.ds(0, tiles)], local_sem.at[1]),
        pltpu.make_async_copy(noise_hbm, noise, local_sem.at[2]),
        pltpu.make_async_copy(lead_hbm, lead, local_sem.at[3]),
    ]
    past = [
        pltpu.make_async_copy(
            history_hbm.at[:, :, pl.ds(i * piece_len, piece_len)],
            hist.at[pl.ds(0, cycle_len), i],
            past_sem.at[i],
        )
        for i in range(block_len // piece_len)
    ]
    index = [
        pltpu.make_async_copy(a, b, index_sem.at[i])
        for i, (a, b) in enumerate(
            ((group_hbm, src_group), (sub_hbm, src_sub), (delays_hbm, delays), (counts_hbm, counts))
        )
    ]
    for copy in index:
        copy.start()
    for copy in past:
        copy.start()

    greeted = len(remote) + len([1 for d, c in seats if c])

    def choose(block, owner):
        live = counts[block]
        rank = jnp.int32(0)
        found = [jnp.int32(tiles)] * slots
        subs = [jnp.int32(0)] * slots
        starts = [jnp.int32(cycle_len - DMIN)] * slots
        for k in range(tiles):
            hit = jnp.logical_and(src_group[k, block] == owner, k < live)
            sub, start = src_sub[k, block], cycle_len - delays[k, block]
            for r in range(slots):
                take = jnp.logical_and(hit, rank == r)
                found[r] = jnp.where(take, k, found[r])
                subs[r] = jnp.where(take, sub, subs[r])
                starts[r] = jnp.where(take, start, starts[r])
            rank = rank + jnp.where(hit, 1, 0)
        return found, subs, starts

    def choose_out(dest, carry):
        _, subs, starts = choose(dest * columns + column, me)
        for r in range(slots):
            sel_sub[dest * slots + r] = subs[r]
            sel_start[dest * slots + r] = starts[r]
        return carry

    for copy in index:
        copy.wait()
    lax.fori_loop(0, owners, choose_out, 0)

    for copy in past:
        copy.wait()
    for copy in loads:
        copy.start()

    def pack(owner, carry):
        for r in range(slots):
            start, sub = sel_start[owner * slots + r], sel_sub[owner * slots + r]
            for t in range(STEPS):
                staged[owner, t, r] = hist[start + t, sub]
        return carry

    lax.fori_loop(0, owners, pack, 0)

    def parcel(g, p, d):
        times = pl.ds(GROUPS[g][0], len(GROUPS[g]))
        dest = partner(p, d)
        return pltpu.make_async_remote_copy(
            src_ref=staged.at[dest, times],
            dst_ref=landed.at[me, times],
            send_sem=send_sem.at[g, p * INNER + d],
            recv_sem=recv_sem.at[g, p * INNER + d],
            device_id={"grp": dest},
            device_id_type=MESH,
        )

    def issue(g):
        for p, d in remote:
            parcel(g, p, d).start()

    pl.semaphore_wait(barrier, greeted)
    for g in range(AHEAD):
        issue(g)
    loads[0].wait()

    def first_fire(tile, carry):
        cols = pl.ds(pl.multiple_of(tile * piece_len, piece_len), piece_len)
        fire = sigmoid_spike_density(state[1, :, cols] - state[2, :, cols])
        hist[cycle_len, tile] = fire.astype(jnp.bfloat16)
        return carry

    lax.fori_loop(0, block_len // piece_len, first_fire, 0)
    def pack_last(owner, carry):
        for r in range(slots):
            start, sub = sel_start[owner * slots + r], sel_sub[owner * slots + r]
            staged[owner, STEPS, r] = hist[start + STEPS, sub]
        return carry

    lax.fori_loop(0, owners, pack_last, 0)
    landed[me] = staged[me]

    def choose_in(owner, carry):
        found, _, _ = choose(me * columns + column, owner)
        for r in range(slots):
            sel_tile[owner * slots + r] = found[r]
        return carry

    lax.fori_loop(0, owners, choose_in, 0)
    weights[tiles] = jnp.zeros(weights.shape[1:], jnp.bfloat16)
    loads[1].wait()

    def place_weights(place, carry):
        rows = pl.ds(pl.multiple_of(place * piece_len, piece_len), piece_len)
        placed[rows, :] = weights[sel_tile[place]]
        return carry

    lax.fori_loop(0, owners * slots, place_weights, 0)
    loads[2].wait()
    loads[3].wait()
    lead_t[...] = lead[...].T

    group = INNER * slots
    depth = group * piece_len
    dot_cols = min(512, block_len)

    def absorb(g, p):
        for d in range(INNER):
            if (p, d) != (0, 0):
                parcel(g, p, d).wait_recv()
        zone = flip(layer, p)
        lhs = jnp.concatenate(
            [
                jnp.concatenate(
                    [landed[zone * INNER + d, t, r] for d in range(INNER) for r in range(slots)],
                    axis=1,
                )
                for t in GROUPS[g]
            ],
            axis=0,
        )
        out = slice(GROUPS[g][0] * replicas, (GROUPS[g][-1] + 1) * replicas)
        rows = pl.ds(pl.multiple_of(zone * depth, depth), depth)
        for start in range(0, block_len, dot_cols):
            cols = slice(start, start + dot_cols)
            part = jnp.dot(lhs, placed[rows, cols], preferred_element_type=jnp.float32)
            if p == 0:
                coupled[out, cols] = part
            else:
                coupled[out, cols] = coupled[out, cols] + part

    part_rows = 32

    def blocks(body):
        def step(i, carry):
            rows = pl.ds(pl.multiple_of(lax.rem(i, replicas // part_rows) * part_rows, part_rows), part_rows)
            cols = pl.ds(
                pl.multiple_of(lax.div(i, replicas // part_rows) * piece_len, piece_len), piece_len
            )
            body(rows, cols)
            return carry

        lax.fori_loop(0, (replicas // part_rows) * (block_len // piece_len), step, 0)

    def read(rows, cols):
        return [state[i, rows, cols] for i in range(6)]

    def move(t, out):
        def body(rows, cols):
            y = read(rows, cols)
            now = coupled[pl.ds(pl.multiple_of(t * replicas + rows.start, part_rows), part_rows), cols]
            if t > 0:
                y[4] = y[4] + NEXT_GAIN * now
            y = advance(y, noise[rows, cols], now)
            if out is state:
                potential[rows, cols] = (y[1] - y[2]).astype(jnp.bfloat16)
            for i in range(6):
                out[i, rows, cols] = y[i]

        blocks(body)

    def signal():
        return jnp.dot(potential[...], lead_t[...], preferred_element_type=jnp.float32)

    def near_device(d, c):
        return {"grp": partner(0, d), "node": lax.rem(column + c, columns)}

    def full_copy(s, d, c):
        return pltpu.make_async_remote_copy(
            src_ref=full_in.at[s, seat],
            dst_ref=full_in.at[s, seat],
            send_sem=full_send.at[s, d * columns + c],
            recv_sem=full_recv.at[s, d * columns + c],
            device_id=near_device(d, c),
            device_id_type=MESH,
        )

    def full_z_copy(s, p):
        return pltpu.make_async_remote_copy(
            src_ref=full_z.at[s, layer],
            dst_ref=full_z.at[s, layer],
            send_sem=full_z_send.at[s, p],
            recv_sem=full_z_recv.at[s, p],
            device_id={"grp": partner(p, 0)},
            device_id_type=MESH,
        )

    def bulk_copy(d, c):
        other = lax.rem(inside + d, INNER) * columns + lax.rem(column + c, columns)
        return pltpu.make_async_remote_copy(
            src_ref=bulk.at[other],
            dst_ref=bulk_in.at[seat],
            send_sem=bulk_send.at[d * columns + c],
            recv_sem=bulk_recv.at[d * columns + c],
            device_id=near_device(d, c),
            device_id_type=MESH,
        )

    def bulk_z_copy(p):
        return pltpu.make_async_remote_copy(
            src_ref=bulk_z.at[layer],
            dst_ref=bulk_z.at[layer],
            send_sem=bulk_z_send.at[p],
            recv_sem=bulk_z_recv.at[p],
            device_id={"grp": partner(p, 0)},
            device_id_type=MESH,
        )

    def bulk_all_copy(d, c):
        return pltpu.make_async_remote_copy(
            src_ref=bulk_all.at[seat],
            dst_ref=bulk_all.at[seat],
            send_sem=bulk_all_send.at[d * columns + c],
            recv_sem=bulk_all_recv.at[d * columns + c],
            device_id=near_device(d, c),
            device_id_type=MESH,
        )

    def total(ref, count):
        out = ref[0]
        for i in range(1, count):
            out = out + ref[i]
        return out

    layers = list(range(1, outer))

    def start_full(s):
        full_in[s, seat] = signal()
        for d, c in seats:
            full_copy(s, d, c).start()

    def turn_full(s):
        for d, c in seats:
            full_copy(s, d, c).wait_recv()
        full_z[s, layer] = total(full_in.at[s], near)
        for p in layers:
            full_z_copy(s, p).start()

    def end_full(s):
        for p in layers:
            full_z_copy(s, p).wait_recv()
        row = (BULK + s) * replicas
        sensors_out[row : row + replicas, :] = total(full_z.at[s], outer)

    last = len(GROUPS) - 2
    for g in range(last):
        for p in range(outer):
            absorb(g, p)
            if p == STAGE and g + AHEAD <= last:
                issue(g + AHEAD)
        for t in GROUPS[g]:
            move(t, state)
            if t < BULK:
                part = signal()
                for i in range(replicas // share):
                    bulk[t * (replicas // share) + i] = part[i * share : (i + 1) * share, :]
            if t == BULK - 1:
                for d, c in seats:
                    bulk_copy(d, c).start()
                bulk_in[seat] = bulk[seat]
            if t == BULK:
                start_full(0)
                for d, c in seats:
                    bulk_copy(d, c).wait_recv()
                bulk_z[layer] = total(bulk_in, near)
                for p in layers:
                    bulk_z_copy(p).start()

    def ahead(rows, cols):
        y = read(rows, cols)
        y = advance(y, noise[rows, cols], None)
        base[rows, cols] = y[1] - y[2]

    blocks(ahead)
    if HOLD < 0:
        issue(last + 1)

    for p in range(outer):
        absorb(last, p)
        if p == HOLD:
            issue(last + 1)
    at = slice(GROUPS[last][0] * replicas, (GROUPS[last][0] + 1) * replicas)
    potential[...] = (base[...] + POTENTIAL_GAIN * coupled[at, :]).astype(jnp.bfloat16)
    start_full(1)
    if HOLD == outer:
        issue(last + 1)

    turn_full(0)
    for p in layers:
        bulk_z_copy(p).wait_recv()
    bulk_all[seat] = total(bulk_z, outer)
    for d, c in seats:
        bulk_all_copy(d, c).start()
    move(STEPS - 1, final_out)

    absorb(last + 1, 0)
    turn_full(1)
    for p in range(1, outer):
        absorb(last + 1, p)
    at = slice(STEPS * replicas, TIMES * replicas)
    final_out[4] = final_out[4] + NEXT_GAIN * coupled[at, :]

    end_full(0)
    for d, c in seats:
        bulk_all_copy(d, c).wait_recv()
    for i in range(near):
        sensors_out[i * share : (i + 1) * share, :] = bulk_all[i]
    for g in range(len(GROUPS)):
        for p, d in remote:
            parcel(g, p, d).wait_send()
    for d, c in seats:
        bulk_copy(d, c).wait_send()
        bulk_all_copy(d, c).wait_send()
        for s in range(2):
            full_copy(s, d, c).wait_send()
    for p in layers:
        bulk_z_copy(p).wait_send()
        full_z_copy(0, p).wait_send()
    end_full(1)
    for p in layers:
        full_z_copy(1, p).wait_send()


def deliver(state, sensors, state_out, sensors_out, sem):
    copies = [
        pltpu.make_async_copy(sensors, sensors_out, sem.at[0]),
    ] + [
        pltpu.make_async_copy(state.at[i], state_out.at[i], sem.at[1 + i])
        for i in range(state.shape[0])
    ]
    for copy in copies:
        copy.start()
    for copy in copies:
        copy.wait()


def body(
    owners,
    columns,
    initial,
    afferent_noise_level,
    history,
    weights,
    lead_field,
    src_group,
    src_sub,
    delays,
    counts,
):
    cycle_len, replicas, block_len = history.shape
    tiles = src_group.shape[1]
    piece_len = weights.shape[2]
    sensors = lead_field.shape[0]
    slots = (tiles + owners - 1) // owners
    places = owners * slots
    outer = owners // INNER
    near = INNER * columns
    share = BULK * replicas // near
    smem = pl.BlockSpec(memory_space=pltpu.SMEM)
    vmem = pl.BlockSpec(memory_space=pltpu.VMEM)
    anywhere = pl.BlockSpec(memory_space=pl.ANY)
    dma = pltpu.SemaphoreType.DMA
    final, signal = pl.pallas_call(
        functools.partial(kernel, owners, columns, slots),
        out_shape=(
            pltpu.VMEM(initial.shape, jnp.float32),
            pltpu.VMEM((STEPS * replicas, sensors), jnp.float32),
        ),
        in_specs=[pl.BlockSpec(memory_space=pltpu.HBM)] * 9,
        out_specs=(vmem, vmem),
        scratch_shapes=[
            pltpu.SMEM((tiles, src_group.shape[0]), jnp.int32),
            pltpu.SMEM((tiles, src_group.shape[0]), jnp.int32),
            pltpu.SMEM((tiles, src_group.shape[0]), jnp.int32),
            pltpu.SMEM(counts.shape, jnp.int32),
            dma((4,)),
            pltpu.SMEM((places,), jnp.int32),
            pltpu.SMEM((places,), jnp.int32),
            pltpu.SMEM((places,), jnp.int32),
            pltpu.VMEM((cycle_len + 1, block_len // piece_len, replicas, piece_len), jnp.bfloat16),
            pltpu.VMEM(initial.shape, jnp.float32),
            pltpu.VMEM((replicas, block_len), jnp.float32),
            pltpu.VMEM((tiles + 1, piece_len, block_len), jnp.bfloat16),
            pltpu.VMEM((places * piece_len, block_len), jnp.bfloat16),
            pltpu.VMEM(lead_field.shape, jnp.bfloat16),
            pltpu.VMEM((block_len, sensors), jnp.bfloat16),
            pltpu.VMEM((owners, TIMES, slots, replicas, piece_len), jnp.bfloat16),
            pltpu.VMEM((owners, TIMES, slots, replicas, piece_len), jnp.bfloat16),
            pltpu.VMEM((TIMES * replicas, block_len), jnp.float32),
            pltpu.VMEM((replicas, block_len), jnp.float32),
            pltpu.VMEM((replicas, block_len), jnp.bfloat16),
            pltpu.VMEM((near, share, sensors), jnp.float32),
            pltpu.VMEM((near, share, sensors), jnp.float32),
            pltpu.VMEM((outer, share, sensors), jnp.float32),
            pltpu.VMEM((near, share, sensors), jnp.float32),
            pltpu.VMEM((2, near, replicas, sensors), jnp.float32),
            pltpu.VMEM((2, outer, replicas, sensors), jnp.float32),
            dma((4,)),
            dma((block_len // piece_len,)),
            dma((len(GROUPS), owners)),
            dma((len(GROUPS), owners)),
            dma((near,)),
            dma((near,)),
            dma((outer,)),
            dma((outer,)),
            dma((near,)),
            dma((near,)),
            dma((2, near)),
            dma((2, near)),
            dma((2, outer)),
            dma((2, outer)),
        ],
        compiler_params=pltpu.CompilerParams(
            collective_id=0, has_side_effects=True, vmem_limit_bytes=VMEM_BYTES
        ),
    )(
        *(
            pltpu.with_memory_space_constraint(array, pltpu.HBM)
            for array in (
                src_group.T,
                src_sub.T,
                delays.T,
                counts,
                initial,
                afferent_noise_level,
                history,
                weights.reshape(tiles, piece_len, block_len),
                lead_field,
            )
        ),
    )
    final, signal = pl.pallas_call(
        deliver,
        out_shape=(
            jax.ShapeDtypeStruct(final.shape, jnp.float32),
            jax.ShapeDtypeStruct(signal.shape, jnp.float32),
        ),
        in_specs=[vmem, vmem],
        out_specs=(anywhere, anywhere),
        scratch_shapes=[dma((1 + final.shape[0],))],
        compiler_params=pltpu.CompilerParams(vmem_limit_bytes=8 * 1024 * 1024),
    )(
        pltpu.with_memory_space_constraint(final, pltpu.VMEM),
        pltpu.with_memory_space_constraint(signal, pltpu.VMEM),
    )
    signal = signal.reshape(STEPS, replicas, sensors)
    return final, jnp.transpose(signal, (0, 2, 1))


def solution(mesh):
    return jax.shard_map(
        functools.partial(body, mesh.shape["grp"], mesh.shape["node"]),
        mesh=mesh,
        in_specs=(
            P(None, None, ("grp", "node")),
            P(None, ("grp", "node")),
            P(None, None, ("grp", "node")),
            P(("grp", "node"), None, None, None),
            P(None, ("grp", "node")),
            P(),
            P(),
            P(),
            P(),
        ),
        out_specs=(P(None, None, ("grp", "node")), P()),
        check_vma=False,
    )
```

```python
import functools

import jax
import jax.numpy as jnp
from jax import lax
from jax.experimental import pallas as pl
from jax.experimental.pallas import tpu as pltpu
from jax.sharding import PartitionSpec as P

DMIN = 6
STEPS = 6
TIMES = STEPS + 1
BULK = 4
INNER = 2
GROUPS = ((0,), (1, 2), (3,), (4,), (5,), (6,))
AHEAD = 2
STAGE = 2
HOLD = 2
VMEM_BYTES = 40 * 1024 * 1024

exciting_amplitude = 3.25
suppressive_amplitude = 22.0
exciting_inverse_lag = 0.1
suppressive_inverse_lag = 0.05
link_factor = 135.0
maximal_spike_frequency = 0.005
thresh = 6.0
fire_slope = 0.56
global_scaling_factor = 0.5
dt_step = 0.5

COUPLED_RATE = exciting_amplitude * exciting_inverse_lag * global_scaling_factor
NEXT_GAIN = 0.5 * dt_step * COUPLED_RATE
POTENTIAL_GAIN = (
    0.5
    * dt_step
    * (2.0 * NEXT_GAIN + dt_step * (COUPLED_RATE - 2.0 * exciting_inverse_lag * NEXT_GAIN))
)

MESH = pl.DeviceIdType.MESH


def sigmoid_spike_density(level):
    return 1.0 / (1.0 + jnp.exp(fire_slope * (thresh - level)))


def derivative(y, noise, coupled):
    curvature = (
        exciting_amplitude
        * exciting_inverse_lag
        * maximal_spike_frequency
        * sigmoid_spike_density(y[1] - y[2])
        - 2.0 * exciting_inverse_lag * y[3]
        - exciting_inverse_lag * exciting_inverse_lag * y[0]
    )
    drive = noise + 0.8 * link_factor * maximal_spike_frequency * sigmoid_spike_density(
        link_factor * y[0]
    )
    if coupled is not None:
        drive = drive + global_scaling_factor * coupled
    interneuron = (
        exciting_amplitude * exciting_inverse_lag * drive
        - 2.0 * exciting_inverse_lag * y[4]
        - exciting_inverse_lag * exciting_inverse_lag * y[1]
    )
    suppressive = (
        suppressive_amplitude
        * suppressive_inverse_lag
        * 0.25
        * link_factor
        * maximal_spike_frequency
        * sigmoid_spike_density(0.25 * link_factor * y[0])
        - 2.0 * suppressive_inverse_lag * y[5]
        - suppressive_inverse_lag * suppressive_inverse_lag * y[2]
    )
    return [y[3], y[4], y[5], curvature, interneuron, suppressive]


def advance(y, noise, coupled_now):
    first = derivative(y, noise, coupled_now)
    moved = [a + dt_step * b for a, b in zip(y, first)]
    second = derivative(moved, noise, None)
    return [a + 0.5 * dt_step * (b + c) for a, b, c in zip(y, first, second)]


def flip(index, mask):
    out = index
    bit = 1
    while bit <= mask:
        if mask & bit:
            out = out + bit * (1 - 2 * (lax.div(index, bit) % 2))
        bit *= 2
    return out


def kernel(
    owners,
    columns,
    slots,
    group_hbm,
    sub_hbm,
    delays_hbm,
    counts_hbm,
    initial_hbm,
    noise_hbm,
    history_hbm,
    weights_hbm,
    lead_hbm,
    final_out,
    sensors_out,
    src_group,
    src_sub,
    delays,
    counts,
    index_sem,
    sel_sub,
    sel_start,
    sel_tile,
    hist,
    state,
    noise,
    weights,
    placed,
    lead,
    lead_t,
    staged,
    landed,
    coupled,
    base,
    potential,
    bulk,
    bulk_in,
    bulk_z,
    bulk_all,
    full_in,
    full_z,
    local_sem,
    past_sem,
    send_sem,
    recv_sem,
    bulk_send,
    bulk_recv,
    bulk_z_send,
    bulk_z_recv,
    bulk_all_send,
    bulk_all_recv,
    full_send,
    full_recv,
    full_z_send,
    full_z_recv,
):
    me = lax.axis_index("grp")
    column = lax.axis_index("node")
    outer = owners // INNER
    layer = lax.div(me, INNER)
    inside = lax.rem(me, INNER)
    near = INNER * columns
    seat = inside * columns + column
    tiles = src_group.shape[0]
    cycle_len, replicas, block_len = history_hbm.shape
    piece_len = weights.shape[1]
    share = bulk.shape[1]

    def partner(p, d):
        return flip(layer, p) * INNER + lax.rem(inside + d, INNER)

    pairs = [(p, d) for p in range(outer - 1, -1, -1) for d in range(INNER)]
    remote = [(p, d) for p, d in pairs if (p, d) != (0, 0)]
    seats = [(d, c) for d in range(INNER) for c in range(columns) if (d, c) != (0, 0)]

    barrier = pltpu.get_barrier_semaphore()
    for p, d in remote:
        pl.semaphore_signal(
            barrier, inc=1, device_id={"grp": partner(p, d)}, device_id_type=MESH
        )
    for d, c in seats:
        if c:
            pl.semaphore_signal(
                barrier,
                inc=1,
                device_id={"grp": partner(0, d), "node": lax.rem(column + c, columns)},
                device_id_type=MESH,
            )
    loads = [
        pltpu.make_async_copy(initial_hbm, state, local_sem.at[0]),
        pltpu.make_async_copy(weights_hbm, weights.at[pl.ds(0, tiles)], local_sem.at[1]),
        pltpu.make_async_copy(noise_hbm, noise, local_sem.at[2]),
        pltpu.make_async_copy(lead_hbm, lead, local_sem.at[3]),
    ]
    past = [
        pltpu.make_async_copy(
            history_hbm.at[:, :, pl.ds(i * piece_len, piece_len)],
            hist.at[pl.ds(0, cycle_len), i],
            past_sem.at[i],
        )
        for i in range(block_len // piece_len)
    ]
    index = [
        pltpu.make_async_copy(a, b, index_sem.at[i])
        for i, (a, b) in enumerate(
            ((group_hbm, src_group), (sub_hbm, src_sub), (delays_hbm, delays), (counts_hbm, counts))
        )
    ]
    for copy in index:
        copy.start()
    for copy in past:
        copy.start()

    greeted = len(remote) + len([1 for d, c in seats if c])

    def choose(block, owner):
        live = counts[block]
        rank = jnp.int32(0)
        found = [jnp.int32(tiles)] * slots
        subs = [jnp.int32(0)] * slots
        starts = [jnp.int32(cycle_len - DMIN)] * slots
        for k in range(tiles):
            hit = jnp.logical_and(src_group[k, block] == owner, k < live)
            sub, start = src_sub[k, block], cycle_len - delays[k, block]
            for r in range(slots):
                take = jnp.logical_and(hit, rank == r)
                found[r] = jnp.where(take, k, found[r])
                subs[r] = jnp.where(take, sub, subs[r])
                starts[r] = jnp.where(take, start, starts[r])
            rank = rank + jnp.where(hit, 1, 0)
        return found, subs, starts

    def choose_out(dest, carry):
        _, subs, starts = choose(dest * columns + column, me)
        for r in range(slots):
            sel_sub[dest * slots + r] = subs[r]
            sel_start[dest * slots + r] = starts[r]
        return carry

    for copy in index:
        copy.wait()
    lax.fori_loop(0, owners, choose_out, 0)

    for copy in past:
        copy.wait()
    for copy in loads:
        copy.start()

    def pack(owner, carry):
        for r in range(slots):
            start, sub = sel_start[owner * slots + r], sel_sub[owner * slots + r]
            for t in range(STEPS):
                staged[owner, t, r] = hist[start + t, sub]
        return carry

    lax.fori_loop(0, owners, pack, 0)

    def parcel(g, p, d):
        times = pl.ds(GROUPS[g][0], len(GROUPS[g]))
        dest = partner(p, d)
        return pltpu.make_async_remote_copy(
            src_ref=staged.at[dest, times],
            dst_ref=landed.at[me, times],
            send_sem=send_sem.at[g, p * INNER + d],
            recv_sem=recv_sem.at[g, p * INNER + d],
            device_id={"grp": dest},
            device_id_type=MESH,
        )

    def issue(g):
        for p, d in remote:
            parcel(g, p, d).start()

    pl.semaphore_wait(barrier, greeted)
    for g in range(AHEAD):
        issue(g)
    loads[0].wait()

    def first_fire(tile, carry):
        cols = pl.ds(pl.multiple_of(tile * piece_len, piece_len), piece_len)
        fire = sigmoid_spike_density(state[1, :, cols] - state[2, :, cols])
        hist[cycle_len, tile] = fire.astype(jnp.bfloat16)
        return carry

    lax.fori_loop(0, block_len // piece_len, first_fire, 0)
    def pack_last(owner, carry):
        for r in range(slots):
            start, sub = sel_start[owner * slots + r], sel_sub[owner * slots + r]
            staged[owner, STEPS, r] = hist[start + STEPS, sub]
        return carry

    lax.fori_loop(0, owners, pack_last, 0)
    landed[me] = staged[me]

    def choose_in(owner, carry):
        found, _, _ = choose(me * columns + column, owner)
        for r in range(slots):
            sel_tile[owner * slots + r] = found[r]
        return carry

    lax.fori_loop(0, owners, choose_in, 0)
    weights[tiles] = jnp.zeros(weights.shape[1:], jnp.bfloat16)
    loads[1].wait()

    def place_weights(place, carry):
        rows = pl.ds(pl.multiple_of(place * piece_len, piece_len), piece_len)
        placed[rows, :] = weights[sel_tile[place]]
        return carry

    lax.fori_loop(0, owners * slots, place_weights, 0)
    loads[2].wait()
    loads[3].wait()
    lead_t[...] = lead[...].T

    group = INNER * slots
    depth = group * piece_len
    dot_cols = min(512, block_len)

    def absorb(g, p):
        for d in range(INNER):
            if (p, d) != (0, 0):
                parcel(g, p, d).wait_recv()
        zone = flip(layer, p)
        lhs = jnp.concatenate(
            [
                jnp.concatenate(
                    [landed[zone * INNER + d, t, r] for d in range(INNER) for r in range(slots)],
                    axis=1,
                )
                for t in GROUPS[g]
            ],
            axis=0,
        )
        out = slice(GROUPS[g][0] * replicas, (GROUPS[g][-1] + 1) * replicas)
        rows = pl.ds(pl.multiple_of(zone * depth, depth), depth)
        for start in range(0, block_len, dot_cols):
            cols = slice(start, start + dot_cols)
            part = jnp.dot(lhs, placed[rows, cols], preferred_element_type=jnp.float32)
            if p == 0:
                coupled[out, cols] = part
            else:
                coupled[out, cols] = coupled[out, cols] + part

    part_rows = 32

    def blocks(body):
        def step(i, carry):
            rows = pl.ds(pl.multiple_of(lax.rem(i, replicas // part_rows) * part_rows, part_rows), part_rows)
            cols = pl.ds(
                pl.multiple_of(lax.div(i, replicas // part_rows) * piece_len, piece_len), piece_len
            )
            body(rows, cols)
            return carry

        lax.fori_loop(0, (replicas // part_rows) * (block_len // piece_len), step, 0)

    def read(rows, cols):
        return [state[i, rows, cols] for i in range(6)]

    def move(t, out):
        def body(rows, cols):
            y = read(rows, cols)
            now = coupled[pl.ds(pl.multiple_of(t * replicas + rows.start, part_rows), part_rows), cols]
            if t > 0:
                y[4] = y[4] + NEXT_GAIN * now
            y = advance(y, noise[rows, cols], now)
            if out is state:
                potential[rows, cols] = (y[1] - y[2]).astype(jnp.bfloat16)
            for i in range(6):
                out[i, rows, cols] = y[i]

        blocks(body)

    def signal():
        return jnp.dot(potential[...], lead_t[...], preferred_element_type=jnp.float32)

    def near_device(d, c):
        return {"grp": partner(0, d), "node": lax.rem(column + c, columns)}

    def full_copy(s, d, c):
        return pltpu.make_async_remote_copy(
            src_ref=full_in.at[s, seat],
            dst_ref=full_in.at[s, seat],
            send_sem=full_send.at[s, d * columns + c],
            recv_sem=full_recv.at[s, d * columns + c],
            device_id=near_device(d, c),
            device_id_type=MESH,
        )

    def full_z_copy(s, p):
        return pltpu.make_async_remote_copy(
            src_ref=full_z.at[s, layer],
            dst_ref=full_z.at[s, layer],
            send_sem=full_z_send.at[s, p],
            recv_sem=full_z_recv.at[s, p],
            device_id={"grp": partner(p, 0)},
            device_id_type=MESH,
        )

    def bulk_copy(d, c):
        other = lax.rem(inside + d, INNER) * columns + lax.rem(column + c, columns)
        return pltpu.make_async_remote_copy(
            src_ref=bulk.at[other],
            dst_ref=bulk_in.at[seat],
            send_sem=bulk_send.at[d * columns + c],
            recv_sem=bulk_recv.at[d * columns + c],
            device_id=near_device(d, c),
            device_id_type=MESH,
        )

    def bulk_z_copy(p):
        return pltpu.make_async_remote_copy(
            src_ref=bulk_z.at[layer],
            dst_ref=bulk_z.at[layer],
            send_sem=bulk_z_send.at[p],
            recv_sem=bulk_z_recv.at[p],
            device_id={"grp": partner(p, 0)},
            device_id_type=MESH,
        )

    def bulk_all_copy(d, c):
        return pltpu.make_async_remote_copy(
            src_ref=bulk_all.at[seat],
            dst_ref=bulk_all.at[seat],
            send_sem=bulk_all_send.at[d * columns + c],
            recv_sem=bulk_all_recv.at[d * columns + c],
            device_id=near_device(d, c),
            device_id_type=MESH,
        )

    def total(ref, count):
        out = ref[0]
        for i in range(1, count):
            out = out + ref[i]
        return out

    layers = list(range(1, outer))

    def start_full(s):
        full_in[s, seat] = signal()
        for d, c in seats:
            full_copy(s, d, c).start()

    def turn_full(s):
        for d, c in seats:
            full_copy(s, d, c).wait_recv()
        full_z[s, layer] = total(full_in.at[s], near)
        for p in layers:
            full_z_copy(s, p).start()

    def end_full(s):
        for p in layers:
            full_z_copy(s, p).wait_recv()
        row = (BULK + s) * replicas
        sensors_out[row : row + replicas, :] = total(full_z.at[s], outer)

    last = len(GROUPS) - 2
    for g in range(last):
        for p in range(outer):
            absorb(g, p)
            if p == STAGE and g + AHEAD <= last:
                issue(g + AHEAD)
        for t in GROUPS[g]:
            move(t, state)
            if t < BULK:
                part = signal()
                for i in range(replicas // share):
                    bulk[t * (replicas // share) + i] = part[i * share : (i + 1) * share, :]
            if t == BULK - 1:
                for d, c in seats:
                    bulk_copy(d, c).start()
                bulk_in[seat] = bulk[seat]
            if t == BULK:
                start_full(0)
                for d, c in seats:
                    bulk_copy(d, c).wait_recv()
                bulk_z[layer] = total(bulk_in, near)
                for p in layers:
                    bulk_z_copy(p).start()

    def ahead(rows, cols):
        y = read(rows, cols)
        y = advance(y, noise[rows, cols], None)
        base[rows, cols] = y[1] - y[2]

    blocks(ahead)
    if HOLD < 0:
        issue(last + 1)

    for p in range(outer):
        absorb(last, p)
        if p == HOLD:
            issue(last + 1)
    at = slice(GROUPS[last][0] * replicas, (GROUPS[last][0] + 1) * replicas)
    potential[...] = (base[...] + POTENTIAL_GAIN * coupled[at, :]).astype(jnp.bfloat16)
    start_full(1)
    if HOLD == outer:
        issue(last + 1)

    turn_full(0)
    move(STEPS - 1, final_out)

    absorb(last + 1, 0)
    turn_full(1)
    for p in layers:
        bulk_z_copy(p).wait_recv()
    bulk_all[seat] = total(bulk_z, outer)
    for d, c in seats:
        bulk_all_copy(d, c).start()
    for p in range(1, outer):
        absorb(last + 1, p)
    at = slice(STEPS * replicas, TIMES * replicas)
    final_out[4] = final_out[4] + NEXT_GAIN * coupled[at, :]

    end_full(0)
    for d, c in seats:
        bulk_all_copy(d, c).wait_recv()
    for i in range(near):
        sensors_out[i * share : (i + 1) * share, :] = bulk_all[i]
    for g in range(len(GROUPS)):
        for p, d in remote:
            parcel(g, p, d).wait_send()
    for d, c in seats:
        bulk_copy(d, c).wait_send()
        bulk_all_copy(d, c).wait_send()
        for s in range(2):
            full_copy(s, d, c).wait_send()
    for p in layers:
        bulk_z_copy(p).wait_send()
        full_z_copy(0, p).wait_send()
    end_full(1)
    for p in layers:
        full_z_copy(1, p).wait_send()


def deliver(state, sensors, state_out, sensors_out, sem):
    copies = [
        pltpu.make_async_copy(sensors, sensors_out, sem.at[0]),
    ] + [
        pltpu.make_async_copy(state.at[i], state_out.at[i], sem.at[1 + i])
        for i in range(state.shape[0])
    ]
    for copy in copies:
        copy.start()
    for copy in copies:
        copy.wait()


def body(
    owners,
    columns,
    initial,
    afferent_noise_level,
    history,
    weights,
    lead_field,
    src_group,
    src_sub,
    delays,
    counts,
):
    cycle_len, replicas, block_len = history.shape
    tiles = src_group.shape[1]
    piece_len = weights.shape[2]
    sensors = lead_field.shape[0]
    slots = (tiles + owners - 1) // owners
    places = owners * slots
    outer = owners // INNER
    near = INNER * columns
    share = BULK * replicas // near
    smem = pl.BlockSpec(memory_space=pltpu.SMEM)
    vmem = pl.BlockSpec(memory_space=pltpu.VMEM)
    anywhere = pl.BlockSpec(memory_space=pl.ANY)
    dma = pltpu.SemaphoreType.DMA
    final, signal = pl.pallas_call(
        functools.partial(kernel, owners, columns, slots),
        out_shape=(
            pltpu.VMEM(initial.shape, jnp.float32),
            pltpu.VMEM((STEPS * replicas, sensors), jnp.float32),
        ),
        in_specs=[pl.BlockSpec(memory_space=pltpu.HBM)] * 9,
        out_specs=(vmem, vmem),
        scratch_shapes=[
            pltpu.SMEM((tiles, src_group.shape[0]), jnp.int32),
            pltpu.SMEM((tiles, src_group.shape[0]), jnp.int32),
            pltpu.SMEM((tiles, src_group.shape[0]), jnp.int32),
            pltpu.SMEM(counts.shape, jnp.int32),
            dma((4,)),
            pltpu.SMEM((places,), jnp.int32),
            pltpu.SMEM((places,), jnp.int32),
            pltpu.SMEM((places,), jnp.int32),
            pltpu.VMEM((cycle_len + 1, block_len // piece_len, replicas, piece_len), jnp.bfloat16),
            pltpu.VMEM(initial.shape, jnp.float32),
            pltpu.VMEM((replicas, block_len), jnp.float32),
            pltpu.VMEM((tiles + 1, piece_len, block_len), jnp.bfloat16),
            pltpu.VMEM((places * piece_len, block_len), jnp.bfloat16),
            pltpu.VMEM(lead_field.shape, jnp.bfloat16),
            pltpu.VMEM((block_len, sensors), jnp.bfloat16),
            pltpu.VMEM((owners, TIMES, slots, replicas, piece_len), jnp.bfloat16),
            pltpu.VMEM((owners, TIMES, slots, replicas, piece_len), jnp.bfloat16),
            pltpu.VMEM((TIMES * replicas, block_len), jnp.float32),
            pltpu.VMEM((replicas, block_len), jnp.float32),
            pltpu.VMEM((replicas, block_len), jnp.bfloat16),
            pltpu.VMEM((near, share, sensors), jnp.float32),
            pltpu.VMEM((near, share, sensors), jnp.float32),
            pltpu.VMEM((outer, share, sensors), jnp.float32),
            pltpu.VMEM((near, share, sensors), jnp.float32),
            pltpu.VMEM((2, near, replicas, sensors), jnp.float32),
            pltpu.VMEM((2, outer, replicas, sensors), jnp.float32),
            dma((4,)),
            dma((block_len // piece_len,)),
            dma((len(GROUPS), owners)),
            dma((len(GROUPS), owners)),
            dma((near,)),
            dma((near,)),
            dma((outer,)),
            dma((outer,)),
            dma((near,)),
            dma((near,)),
            dma((2, near)),
            dma((2, near)),
            dma((2, outer)),
            dma((2, outer)),
        ],
        compiler_params=pltpu.CompilerParams(
            collective_id=0, has_side_effects=True, vmem_limit_bytes=VMEM_BYTES
        ),
    )(
        *(
            pltpu.with_memory_space_constraint(array, pltpu.HBM)
            for array in (
                src_group.T,
                src_sub.T,
                delays.T,
                counts,
                initial,
                afferent_noise_level,
                history,
                weights.reshape(tiles, piece_len, block_len),
                lead_field,
            )
        ),
    )
    final, signal = pl.pallas_call(
        deliver,
        out_shape=(
            jax.ShapeDtypeStruct(final.shape, jnp.float32),
            jax.ShapeDtypeStruct(signal.shape, jnp.float32),
        ),
        in_specs=[vmem, vmem],
        out_specs=(anywhere, anywhere),
        scratch_shapes=[dma((1 + final.shape[0],))],
        compiler_params=pltpu.CompilerParams(vmem_limit_bytes=8 * 1024 * 1024),
    )(
        pltpu.with_memory_space_constraint(final, pltpu.VMEM),
        pltpu.with_memory_space_constraint(signal, pltpu.VMEM),
    )
    signal = signal.reshape(STEPS, replicas, sensors)
    return final, jnp.transpose(signal, (0, 2, 1))


def solution(mesh):
    return jax.shard_map(
        functools.partial(body, mesh.shape["grp"], mesh.shape["node"]),
        mesh=mesh,
        in_specs=(
            P(None, None, ("grp", "node")),
            P(None, ("grp", "node")),
            P(None, None, ("grp", "node")),
            P(("grp", "node"), None, None, None),
            P(None, ("grp", "node")),
            P(),
            P(),
            P(),
            P(),
        ),
        out_specs=(P(None, None, ("grp", "node")), P()),
        check_vma=False,
    )
```
